32 devices in a mesh: grp: 2 (over y), blk: 8 (over z, x), uly: 2 (over core).
Axes of the slice: x: 2, y: 2, z: 4, core: 2. Of those that a mesh axis runs over, the one named last changes fastest.
Arguments:
- query: bfloat16 [512, 1152], P(('grp', 'blk', 'uly')), parts along dimension 0, may hold values from -6 to 6
- key: bfloat16 [512, 1152], P(('grp', 'blk', 'uly')), parts along dimension 0, may hold values from -6 to 6
- value: bfloat16 [512, 1152], P(('grp', 'blk', 'uly')), parts along dimension 0, may hold values from -6 to 6
- q_gain: float32 [96], replicated, may hold values from 1 to 2.5
- k_gain: float32 [96], replicated, may hold values from 1 to 2.5
- out_weight: bfloat16 [1152, 2304], P('uly'), may hold values from -0.1875 to 0.1875
Outputs:
- mixed: bfloat16 [512, 2304], P(('grp', 'blk', 'uly')), parts along dimension 0
The draws below stay inside these ranges and needn't reach their ends.
There are 2 independent parts, one for each index of `grp`. The reference program is written for one: setup_inputs(seed, part) draws one part's arguments, and reference() takes and returns one part's arrays. A program takes and returns all parts, laid end to end along the dimension named above; an argument that names none is the same for every part. Nothing has to cross between parts.
All inputs are finite; a program needn't handle non-finite values.
Results may differ from the reference program's by a relative error of at most 0.012.
Values may be sent and summed in bfloat16 or wider, within the bound.
No kernel may reach another device: no remote copies, remote signals or barrier semaphores. Data moves between devices by JAX's collectives and lax.ppermute only.
A program may use at most 128 MiB of HBM per device.

```python
import jax
import jax.numpy as jnp
from jax import lax

H = 12
HD = 96
D = 2304
S = 256


def steps_of(stream_key, extent, pieces, least, top_value):
    def one(position, shards_of):
        heights = jax.random.uniform(jax.random.fold_in(jax.random.fold_in(stream_key, 6), position), (shards_of,), jnp.float32, least / len(pieces), top_value / len(pieces))
        return jnp.repeat(jnp.exp(heights), extent[position] // shards_of).reshape((-1,) + (1,) * (len(extent) - position - 1))

    level = one(*pieces[0])
    for cut in pieces[1:]:
        level = level * one(*cut)
    return level


def normal_values(rng, shape, spread, most, shards=(), dtype=jnp.bfloat16):
    loudness = steps_of(rng, shape, shards, -0.22, 0.18) if shards else 1.0
    drawn = jax.random.normal(rng, shape, jnp.float32) * spread * loudness
    return jnp.minimum(jnp.maximum(drawn, -most), most).astype(dtype)


def setup_inputs(seed: int = 0, part: int = 0) -> dict:
    seeds = jax.random.split(jax.random.key(seed), 7)
    part_splits = jax.random.split(jax.random.fold_in(seeds[6], part), 7)
    query = normal_values(part_splits[0], (S, H * HD), 1.0, 6.0, ((0, 16),))
    key = normal_values(part_splits[1], (S, H * HD), 1.0, 6.0, ((0, 16),))
    value = normal_values(part_splits[2], (S, H * HD), 1.0, 6.0, ((0, 16),))
    q_gain = jnp.clip(jax.random.uniform(seeds[3], (HD,), jnp.float32, 1.0, 2.5), 1.0, 2.5)
    k_gain = jnp.clip(jax.random.uniform(seeds[4], (HD,), jnp.float32, 1.0, 2.5), 1.0, 2.5)
    out_weight = normal_values(seeds[5], (H * HD, D), (H * HD) ** -0.5, 0.1875, ((0, 2),))
    return {"query": query, "key": key, "value": value, "q_gain": q_gain, "k_gain": k_gain, "out_weight": out_weight}


def normed(data, gain):
    count = data.shape[0]
    grid = data.astype(jnp.float32).reshape(count, H, HD)
    meansq = lax.optimization_barrier(jnp.mean(grid * grid, axis=-1, keepdims=True))
    return (grid * lax.rsqrt(meansq + 1e-06) * gain).astype(jnp.bfloat16)

def reference(query, key, value, q_gain, k_gain, out_weight):
    count = query.shape[0]
    query_heads = jnp.transpose(normed(query, q_gain), (1, 0, 2))
    key_heads = jnp.transpose(normed(key, k_gain), (1, 0, 2))
    value_heads = jnp.transpose(value.reshape(count, H, HD), (1, 0, 2))
    score_scale = float(HD) ** (-0.5)

    def one_head(operands):
        query_one, key_one, value_one = operands
        scores = jnp.dot(query_one, key_one.T, preferred_element_type=jnp.float32) * score_scale
        expd = jnp.exp(scores)
        total_weight = lax.optimization_barrier(jnp.sum(expd, axis=1))
        weighted = jnp.dot(expd.astype(jnp.bfloat16), value_one, preferred_element_type=jnp.float32)
        return (weighted / total_weight[:, None]).astype(jnp.bfloat16)
    attn = lax.map(one_head, (query_heads, key_heads, value_heads))
    attn = jnp.transpose(attn, (1, 0, 2)).reshape(count, H * HD)
    return jnp.dot(attn, out_weight, preferred_element_type=jnp.float32).astype(jnp.bfloat16)
```

```python
import jax
import jax.numpy as jnp
from jax import lax
from jax.experimental import pallas as pl
from jax.experimental.pallas import tpu as pltpu
from jax.sharding import PartitionSpec as P

H = 12
HD = 96
DIRECT = 8


def swap(block, axis, mask):
    count = lax.axis_size(axis)
    return lax.ppermute(block, axis, [(i, i ^ mask) for i in range(count)])


def head_of(rows, width):
    lane = lax.broadcasted_iota(jnp.int32, (rows, width), 1)
    first = lax.broadcasted_iota(jnp.int32, (rows, width), 0) * HD
    return (lane >= first) & (lane < first + HD)


def lane_of(width, cols):
    lane = lax.broadcasted_iota(jnp.int32, (width, cols), 0)
    first = lax.broadcasted_iota(jnp.int32, (width, cols), 1) * HD
    return (lane >= first) & (lane < first + HD)


def pieces(value, count):
    out = []
    for _ in range(count):
        part = value.astype(jnp.bfloat16)
        out.append(part)
        value = value - part.astype(jnp.float32)
    return out


def dot(a, b):
    return jnp.dot(a, b, preferred_element_type=jnp.float32)


def normed_rows(data, gain, gather, spread):
    grid = data.astype(jnp.float32)
    square = sum(dot(part, gather) for part in pieces(grid * grid, 2))
    inverse = lax.rsqrt(square * (1.0 / HD) + 1e-06)
    wide = sum(dot(part, spread) for part in pieces(inverse, 3))
    return (grid * wide * gain).astype(jnp.bfloat16)


def attend_kernel(q_ref, mine_ref, theirs_ref, gain_ref, out_ref):
    rows, width = q_ref.shape
    gather = lane_of(width, 128).astype(jnp.bfloat16)
    spread = head_of(128, width).astype(jnp.bfloat16)
    key = jnp.concatenate([mine_ref[:, :width], theirs_ref[:, :width]], 0)
    value = jnp.concatenate([mine_ref[:, width:], theirs_ref[:, width:]], 0)
    query_n = normed_rows(q_ref[...], gain_ref[0:1, :], gather, spread)
    key_n = normed_rows(key, gain_ref[1:2, :], gather, spread)
    lane = lax.broadcasted_iota(jnp.int32, (rows, width), 1)
    masks = [(lane >= h * HD) & (lane < (h + 1) * HD) for h in range(H)]
    query_f = query_n.astype(jnp.float32)
    stacked = jnp.concatenate([jnp.where(m, query_f, 0.0) for m in masks], 0).astype(jnp.bfloat16)
    scores = lax.dot_general(
        stacked, key_n, (((1,), (1,)), ((), ())), preferred_element_type=jnp.float32
    ) * (float(HD) ** (-0.5))
    expd = jnp.exp(scores)
    total = jnp.sum(expd, axis=1, keepdims=True)
    weighted = dot(expd.astype(jnp.bfloat16), value)
    top = jnp.zeros((rows, width), jnp.float32)
    below = jnp.zeros((rows, width), jnp.float32)
    for h in range(H):
        top = jnp.where(masks[h], weighted[h * rows : (h + 1) * rows], top)
        below = jnp.where(masks[h], total[h * rows : (h + 1) * rows], below)
    out_ref[...] = (top / below).astype(out_ref.dtype)


def normed(data, gain):
    tok_rows = data.shape[0]
    grid = data.astype(jnp.float32).reshape(tok_rows, H, HD)
    meansq = jnp.mean(grid * grid, axis=-1, keepdims=True)
    return (grid * lax.rsqrt(meansq + 1e-06) * gain).astype(jnp.bfloat16)


def general(query, key, value, q_gain, k_gain, out_weight):
    rows, width = query.shape
    keys = lax.all_gather(normed(key, k_gain).reshape(rows, width), ("blk", "uly"), axis=0, tiled=True)
    values = lax.all_gather(value, ("blk", "uly"), axis=0, tiled=True)
    keys, values = keys.reshape(-1, H, HD), values.reshape(-1, H, HD)
    scores = jnp.einsum("qhd,khd->hqk", normed(query, q_gain), keys, preferred_element_type=jnp.float32)
    expd = jnp.exp(scores * (float(HD) ** (-0.5)))
    total = jnp.sum(expd, axis=-1).T
    weighted = jnp.einsum(
        "hqk,khd->qhd", expd.astype(jnp.bfloat16), values, preferred_element_type=jnp.float32
    )
    attn = (weighted / total[:, :, None]).astype(jnp.bfloat16).reshape(rows, width)
    weight = lax.all_gather(out_weight, "uly", axis=0, tiled=True)
    return dot(attn, weight).astype(jnp.bfloat16)


def direct(query, key, value, q_gain, k_gain, out_weight):
    rows, width = query.shape
    blocks = lax.axis_size("blk")
    other_weight = swap(out_weight, "uly", 1)
    held = [jnp.concatenate([key, value], 1)]
    held += [swap(held[0], "blk", mask) for mask in range(2, blocks, 2)]
    held += [swap(block, "blk", 1) for block in held]
    mine = jnp.concatenate(held, 0)
    theirs = swap(mine, "uly", 1)
    gains = jnp.stack([jnp.tile(q_gain, H), jnp.tile(k_gain, H)])
    attn = pl.pallas_call(
        attend_kernel,
        out_shape=jax.ShapeDtypeStruct((rows, width), jnp.bfloat16),
        in_specs=[pl.BlockSpec(memory_space=pltpu.VMEM)] * 4,
        out_specs=pl.BlockSpec(memory_space=pltpu.VMEM),
    )(query, mine, theirs, gains)
    half = width // 2
    first = lax.axis_index("uly") == 0
    own = jnp.where(first, attn[:, :half], attn[:, half:])
    other = jnp.where(first, attn[:, half:], attn[:, :half])
    return (dot(own, out_weight) + dot(other, other_weight)).astype(jnp.bfloat16)


def solution(mesh):
    blocks = mesh.shape["blk"]
    small = mesh.shape["uly"] == 2 and 1 < blocks <= DIRECT and blocks & (blocks - 1) == 0
    rows = P(("grp", "blk", "uly"), None)
    return jax.shard_map(
        direct if small else general,
        mesh=mesh,
        in_specs=(rows, rows, rows, P(), P(), P("uly", None)),
        out_specs=rows,
        check_vma=False,
    )
```

```python
import jax
import jax.numpy as jnp
from jax import lax
from jax.experimental import pallas as pl
from jax.experimental.pallas import tpu as pltpu
from jax.sharding import PartitionSpec as P

H = 12
HD = 96
DIRECT = 8


def swap(block, axis, mask):
    count = lax.axis_size(axis)
    return lax.ppermute(block, axis, [(i, i ^ mask) for i in range(count)])


def head_of(rows, width):
    lane = lax.broadcasted_iota(jnp.int32, (rows, width), 1)
    first = lax.broadcasted_iota(jnp.int32, (rows, width), 0) * HD
    return (lane >= first) & (lane < first + HD)


def lane_of(width, cols):
    lane = lax.broadcasted_iota(jnp.int32, (width, cols), 0)
    first = lax.broadcasted_iota(jnp.int32, (width, cols), 1) * HD
    return (lane >= first) & (lane < first + HD)


def pieces(value, count):
    out = []
    for _ in range(count):
        part = value.astype(jnp.bfloat16)
        out.append(part)
        value = value - part.astype(jnp.float32)
    return out


def dot(a, b):
    return jnp.dot(a, b, preferred_element_type=jnp.float32)


def normed_rows(data, gain, gather, spread):
    grid = data.astype(jnp.float32)
    square = sum(dot(part, gather) for part in pieces(grid * grid, 2))
    inverse = lax.rsqrt(square * (1.0 / HD) + 1e-06)
    wide = sum(dot(part, spread) for part in pieces(inverse, 3))
    return (grid * wide * gain).astype(jnp.bfloat16)


def widened(gain):
    channel = lax.broadcasted_iota(jnp.int32, (HD, H * HD), 0)
    lane = lax.broadcasted_iota(jnp.int32, (HD, H * HD), 1)
    hit = lane == channel
    for h in range(1, H):
        hit = hit | (lane == channel + h * HD)
    spread = hit.astype(jnp.bfloat16)
    return sum(dot(part, spread) for part in pieces(gain, 3))


def partial_attention(stacked, held_ref, key_gain, masks, rows):
    width = key_gain.shape[1]
    gather = lane_of(width, 128).astype(jnp.bfloat16)
    spread = head_of(128, width).astype(jnp.bfloat16)
    key_n = normed_rows(held_ref[:, :width], key_gain, gather, spread)
    scores = lax.dot_general(
        stacked, key_n, (((1,), (1,)), ((), ())), preferred_element_type=jnp.float32
    ) * (float(HD) ** (-0.5))
    expd = jnp.exp(scores)
    total = jnp.sum(expd, axis=1, keepdims=True)
    weighted = dot(expd.astype(jnp.bfloat16), held_ref[:, width:])
    top = jnp.zeros((rows, width), jnp.float32)
    below = jnp.zeros((rows, width), jnp.float32)
    for h in range(H):
        top = jnp.where(masks[h], weighted[h * rows : (h + 1) * rows], top)
        below = jnp.where(masks[h], total[h * rows : (h + 1) * rows], below)
    return top, below


def masks_of(rows, width):
    lane = lax.broadcasted_iota(jnp.int32, (rows, width), 1)
    return [(lane >= h * HD) & (lane < (h + 1) * HD) for h in range(H)]


def first_kernel(q_ref, mine_ref, q_gain_ref, k_gain_ref, stacked_ref, gain_ref, top_ref, below_ref):
    rows, width = q_ref.shape
    masks = masks_of(rows, width)
    gather = lane_of(width, 128).astype(jnp.bfloat16)
    spread = head_of(128, width).astype(jnp.bfloat16)
    query_f = normed_rows(q_ref[...], widened(q_gain_ref[...]), gather, spread).astype(jnp.float32)
    stacked = jnp.concatenate([jnp.where(m, query_f, 0.0) for m in masks], 0).astype(jnp.bfloat16)
    key_gain = widened(k_gain_ref[...])
    stacked_ref[...] = stacked
    gain_ref[...] = key_gain
    top_ref[...], below_ref[...] = partial_attention(stacked, mine_ref, key_gain, masks, rows)


def second_kernel(
    theirs_ref, stacked_ref, gain_ref, top_ref, below_ref, own_w_ref, other_w_ref, out_ref
):
    rows, width = top_ref.shape
    masks = masks_of(rows, width)
    top, below = partial_attention(stacked_ref[...], theirs_ref, gain_ref[...], masks, rows)
    attn = (top_ref[...] + top) / (below_ref[...] + below)
    half = width // 2
    low, high = attn[:, :half], attn[:, half:]
    first = lax.axis_index("uly") == 0
    own = jnp.where(first, low, high).astype(jnp.bfloat16)
    other = jnp.where(first, high, low).astype(jnp.bfloat16)
    out_ref[...] = (dot(own, own_w_ref[...]) + dot(other, other_w_ref[...])).astype(out_ref.dtype)


def normed(data, gain):
    tok_rows = data.shape[0]
    grid = data.astype(jnp.float32).reshape(tok_rows, H, HD)
    meansq = jnp.mean(grid * grid, axis=-1, keepdims=True)
    return (grid * lax.rsqrt(meansq + 1e-06) * gain).astype(jnp.bfloat16)


def general(query, key, value, q_gain, k_gain, out_weight):
    rows, width = query.shape
    keys = lax.all_gather(normed(key, k_gain).reshape(rows, width), ("blk", "uly"), axis=0, tiled=True)
    values = lax.all_gather(value, ("blk", "uly"), axis=0, tiled=True)
    keys, values = keys.reshape(-1, H, HD), values.reshape(-1, H, HD)
    scores = jnp.einsum("qhd,khd->hqk", normed(query, q_gain), keys, preferred_element_type=jnp.float32)
    expd = jnp.exp(scores * (float(HD) ** (-0.5)))
    total = jnp.sum(expd, axis=-1).T
    weighted = jnp.einsum(
        "hqk,khd->qhd", expd.astype(jnp.bfloat16), values, preferred_element_type=jnp.float32
    )
    attn = (weighted / total[:, :, None]).astype(jnp.bfloat16).reshape(rows, width)
    weight = lax.all_gather(out_weight, "uly", axis=0, tiled=True)
    return dot(attn, weight).astype(jnp.bfloat16)


def direct(query, key, value, q_gain, k_gain, out_weight):
    rows, width = query.shape
    blocks = lax.axis_size("blk")
    other_weight = swap(out_weight, "uly", 1)
    held = [jnp.concatenate([key, value], 1)]
    held += [swap(held[0], "blk", mask) for mask in range(2, blocks, 2)]
    held += [swap(block, "blk", 1) for block in held]
    mine = jnp.concatenate(held, 0)
    theirs = swap(mine, "uly", 1)
    f32 = jnp.float32
    vmem = pl.BlockSpec(memory_space=pltpu.VMEM)
    cost = pl.CostEstimate(flops=2_000_000_000, bytes_accessed=2 * mine.size, transcendentals=0)
    stacked, gain, top, below = pl.pallas_call(
        first_kernel,
        out_shape=(
            jax.ShapeDtypeStruct((H * rows, width), jnp.bfloat16),
            jax.ShapeDtypeStruct((1, width), f32),
            jax.ShapeDtypeStruct((rows, width), f32),
            jax.ShapeDtypeStruct((rows, width), f32),
        ),
        in_specs=[vmem] * 4,
        out_specs=(vmem,) * 4,
        cost_estimate=cost,
        compiler_params=pltpu.CompilerParams(vmem_limit_bytes=16 << 20),
    )(query, mine, q_gain.reshape(1, HD), k_gain.reshape(1, HD))
    return pl.pallas_call(
        second_kernel,
        out_shape=jax.ShapeDtypeStruct((rows, out_weight.shape[1]), jnp.bfloat16),
        in_specs=[vmem] * 7,
        out_specs=vmem,
        cost_estimate=cost,
        compiler_params=pltpu.CompilerParams(vmem_limit_bytes=24 << 20),
    )(theirs, stacked, gain, top, below, out_weight, other_weight)


def solution(mesh):
    blocks = mesh.shape["blk"]
    small = mesh.shape["uly"] == 2 and 1 < blocks <= DIRECT and blocks & (blocks - 1) == 0
    rows = P(("grp", "blk", "uly"), None)
    return jax.shard_map(
        direct if small else general,
        mesh=mesh,
        in_specs=(rows, rows, rows, P(), P(), P("uly", None)),
        out_specs=rows,
        check_vma=False,
    )
```

```python
import jax
import jax.numpy as jnp
from jax import lax
from jax.experimental import pallas as pl
from jax.experimental.pallas import tpu as pltpu
from jax.sharding import PartitionSpec as P

H = 12
HD = 96
DIRECT = 8


def swap(block, axis, mask):
    count = lax.axis_size(axis)
    return lax.ppermute(block, axis, [(i, i ^ mask) for i in range(count)])


def head_of(rows, width):
    lane = lax.broadcasted_iota(jnp.int32, (rows, width), 1)
    first = lax.broadcasted_iota(jnp.int32, (rows, width), 0) * HD
    return (lane >= first) & (lane < first + HD)


def lane_of(width, cols):
    lane = lax.broadcasted_iota(jnp.int32, (width, cols), 0)
    first = lax.broadcasted_iota(jnp.int32, (width, cols), 1) * HD
    return (lane >= first) & (lane < first + HD)


def pieces(value, count):
    out = []
    for _ in range(count):
        part = value.astype(jnp.bfloat16)
        out.append(part)
        value = value - part.astype(jnp.float32)
    return out


def dot(a, b):
    return jnp.dot(a, b, preferred_element_type=jnp.float32)


def normed_rows(data, gain, gather, spread):
    grid = data.astype(jnp.float32)
    square = sum(dot(part, gather) for part in pieces(grid * grid, 2))
    inverse = lax.rsqrt(square * (1.0 / HD) + 1e-06)
    wide = sum(dot(part, spread) for part in pieces(inverse, 3))
    return (grid * wide * gain).astype(jnp.bfloat16)


def widened(gain):
    channel = lax.broadcasted_iota(jnp.int32, (HD, H * HD), 0)
    lane = lax.broadcasted_iota(jnp.int32, (HD, H * HD), 1)
    hit = lane == channel
    for h in range(1, H):
        hit = hit | (lane == channel + h * HD)
    spread = hit.astype(jnp.bfloat16)
    return sum(dot(part, spread) for part in pieces(gain, 3))


def partial_attention(stacked, held_ref, key_gain, masks, rows):
    width = key_gain.shape[1]
    gather = lane_of(width, 128).astype(jnp.bfloat16)
    spread = head_of(128, width).astype(jnp.bfloat16)
    key_n = normed_rows(held_ref[:, :width], key_gain, gather, spread)
    scores = lax.dot_general(
        stacked, key_n, (((1,), (1,)), ((), ())), preferred_element_type=jnp.float32
    ) * (float(HD) ** (-0.5))
    expd = jnp.exp(scores)
    total = jnp.sum(expd, axis=1, keepdims=True)
    weighted = dot(expd.astype(jnp.bfloat16), held_ref[:, width:])
    top = jnp.zeros((rows, width), jnp.float32)
    below = jnp.zeros((rows, width), jnp.float32)
    for h in range(H):
        top = jnp.where(masks[h], weighted[h * rows : (h + 1) * rows], top)
        below = jnp.where(masks[h], total[h * rows : (h + 1) * rows], below)
    return top, below


def masks_of(rows, width):
    lane = lax.broadcasted_iota(jnp.int32, (rows, width), 1)
    return [(lane >= h * HD) & (lane < (h + 1) * HD) for h in range(H)]


def query_kernel(
    q_any, q_gain_any, k_gain_any, stacked_ref, gain_ref, q_ref, q_gain_ref, k_gain_ref, sems
):
    copies = [
        pltpu.make_async_copy(q_any, q_ref, sems.at[0]),
        pltpu.make_async_copy(q_gain_any, q_gain_ref, sems.at[1]),
        pltpu.make_async_copy(k_gain_any, k_gain_ref, sems.at[2]),
    ]
    for copy in copies:
        copy.start()
    for copy in copies:
        copy.wait()
    rows, width = q_ref.shape
    masks = masks_of(rows, width)
    gather = lane_of(width, 128).astype(jnp.bfloat16)
    spread = head_of(128, width).astype(jnp.bfloat16)
    query_f = normed_rows(q_ref[...], widened(q_gain_ref[...]), gather, spread).astype(jnp.float32)
    stacked = jnp.concatenate([jnp.where(m, query_f, 0.0) for m in masks], 0)
    stacked_ref[...] = stacked.astype(jnp.bfloat16)
    gain_ref[...] = widened(k_gain_ref[...])


def first_kernel(mine_ref, stacked_ref, gain_ref, top_ref, below_ref):
    rows, width = top_ref.shape
    top_ref[...], below_ref[...] = partial_attention(
        stacked_ref[...], mine_ref, gain_ref[...], masks_of(rows, width), rows
    )


def second_kernel(
    theirs_ref, stacked_ref, gain_ref, top_ref, below_ref, own_w_ref, other_w_ref, out_ref
):
    rows, width = top_ref.shape
    masks = masks_of(rows, width)
    top, below = partial_attention(stacked_ref[...], theirs_ref, gain_ref[...], masks, rows)
    attn = (top_ref[...] + top) / (below_ref[...] + below)
    half = width // 2
    low, high = attn[:, :half], attn[:, half:]
    first = lax.axis_index("uly") == 0
    own = jnp.where(first, low, high).astype(jnp.bfloat16)
    other = jnp.where(first, high, low).astype(jnp.bfloat16)
    out_ref[...] = (dot(own, own_w_ref[...]) + dot(other, other_w_ref[...])).astype(out_ref.dtype)


def normed(data, gain):
    tok_rows = data.shape[0]
    grid = data.astype(jnp.float32).reshape(tok_rows, H, HD)
    meansq = jnp.mean(grid * grid, axis=-1, keepdims=True)
    return (grid * lax.rsqrt(meansq + 1e-06) * gain).astype(jnp.bfloat16)


def general(query, key, value, q_gain, k_gain, out_weight):
    rows, width = query.shape
    keys = lax.all_gather(normed(key, k_gain).reshape(rows, width), ("blk", "uly"), axis=0, tiled=True)
    values = lax.all_gather(value, ("blk", "uly"), axis=0, tiled=True)
    keys, values = keys.reshape(-1, H, HD), values.reshape(-1, H, HD)
    scores = jnp.einsum("qhd,khd->hqk", normed(query, q_gain), keys, preferred_element_type=jnp.float32)
    expd = jnp.exp(scores * (float(HD) ** (-0.5)))
    total = jnp.sum(expd, axis=-1).T
    weighted = jnp.einsum(
        "hqk,khd->qhd", expd.astype(jnp.bfloat16), values, preferred_element_type=jnp.float32
    )
    attn = (weighted / total[:, :, None]).astype(jnp.bfloat16).reshape(rows, width)
    weight = lax.all_gather(out_weight, "uly", axis=0, tiled=True)
    return dot(attn, weight).astype(jnp.bfloat16)


def direct(query, key, value, q_gain, k_gain, out_weight):
    rows, width = query.shape
    blocks = lax.axis_size("blk")
    f32 = jnp.float32
    vmem = pl.BlockSpec(memory_space=pltpu.VMEM)
    cost = pl.CostEstimate(flops=2_000_000_000, bytes_accessed=2 * key.size, transcendentals=0)
    limit = pltpu.CompilerParams(vmem_limit_bytes=16 << 20)
    other_weight = swap(out_weight, "uly", 1)
    held = {0: lax.optimization_barrier(jnp.concatenate([key, value], 1))}
    far = blocks // 2
    for mask in [far] * (far > 1) + [1] + [m for m in range(2, blocks, 2) if m != far]:
        held[mask] = swap(held[0], "blk", mask)
    for mask in range(2, blocks, 2):
        held[mask | 1] = swap(held[far], "blk", 1) if mask == far else swap(held[1], "blk", mask)
    stacked, gain = pl.pallas_call(
        query_kernel,
        out_shape=(
            jax.ShapeDtypeStruct((H * rows, width), jnp.bfloat16),
            jax.ShapeDtypeStruct((1, width), f32),
        ),
        in_specs=[pl.BlockSpec(memory_space=pltpu.HBM)] * 3,
        out_specs=(vmem,) * 2,
        scratch_shapes=[
            pltpu.VMEM((rows, width), query.dtype),
            pltpu.VMEM((1, HD), f32),
            pltpu.VMEM((1, HD), f32),
            pltpu.SemaphoreType.DMA((3,)),
        ],
        cost_estimate=cost,
        compiler_params=limit,
    )(query, q_gain.reshape(1, HD), k_gain.reshape(1, HD))
    mine = jnp.concatenate([held[m] for m in range(blocks)], 0)
    mine, stacked, gain = lax.optimization_barrier((mine, stacked, gain))
    theirs = swap(mine, "uly", 1)
    top, below = pl.pallas_call(
        first_kernel,
        out_shape=(jax.ShapeDtypeStruct((rows, width), f32),) * 2,
        in_specs=[vmem] * 3,
        out_specs=(vmem,) * 2,
        cost_estimate=cost,
        compiler_params=limit,
    )(mine, stacked, gain)
    return pl.pallas_call(
        second_kernel,
        out_shape=jax.ShapeDtypeStruct((rows, out_weight.shape[1]), jnp.bfloat16),
        in_specs=[vmem] * 7,
        out_specs=vmem,
        cost_estimate=cost,
        compiler_params=pltpu.CompilerParams(vmem_limit_bytes=24 << 20),
    )(theirs, stacked, gain, top, below, out_weight, other_weight)


def solution(mesh):
    blocks = mesh.shape["blk"]
    small = mesh.shape["uly"] == 2 and 1 < blocks <= DIRECT and blocks & (blocks - 1) == 0
    rows = P(("grp", "blk", "uly"), None)
    return jax.shard_map(
        direct if small else general,
        mesh=mesh,
        in_specs=(rows, rows, rows, P(), P(), P("uly", None)),
        out_specs=rows,
        check_vma=False,
    )
```
